32 devices in a mesh: dp: 4 (over y, core), tensor: 8 (over z, x).
Axes of the slice: x: 2, y: 2, z: 4, core: 2. Of those that a mesh axis runs over, the one named last changes fastest.
Arguments:
- ref_hidden: bfloat16 [1152, 4608], P('dp', 'tensor'), may hold values from -6 to 6
- pol_hidden: bfloat16 [1152, 4608], P('dp', 'tensor'), may hold values from -6 to 6
- readout: bfloat16 [1152, 4608], P('dp', 'tensor'), may hold values from -0.019897461 to 0.019897461
- lengths: int32 [12], P('dp'), may hold values from 16 to 96, as said below
- pairing: int32 [12], replicated, may hold values from 0 to 11, each once
- pre_gain: float32 [4608], replicated, may hold values from 0.25 to 1.75
- post_gain: float32 [4608], replicated, may hold values from 0.25 to 1.75
- w_query: bfloat16 [4608, 4096], P('dp', 'tensor'), may hold values from -0.09375 to 0.09375
- w_key: bfloat16 [4608, 2048], P('dp', 'tensor'), may hold values from -3 to 3
- value_projection: bfloat16 [4608, 2048], P('dp', 'tensor'), may hold values from -0.09375 to 0.09375
- w_out: bfloat16 [4608, 4096], P('dp', 'tensor'), may hold values from -0.09375 to 0.09375
- a_query: bfloat16 [4608, 64], P('dp'), may hold values from -0.09375 to 0.09375
- a_value: bfloat16 [4608, 64], P('dp'), may hold values from -0.09375 to 0.09375
- query_second_factor: bfloat16 [64, 4096], P(None, 'tensor'), may hold values from -0.75 to 0.75
- value_second_factor: bfloat16 [64, 2048], P(None, 'tensor'), may hold values from -0.75 to 0.75
Outputs:
- policy_out: bfloat16 [1152, 4608], P('dp', 'tensor')
- reference_out: bfloat16 [1152, 4608], P('dp', 'tensor')
- dpo_loss: float32 [], replicated
- grad_hidden: bfloat16 [1152, 4608], P('dp', 'tensor')
- grad_a: float32 [4608, 128], P('dp')
- query_factor_gradient: float32 [64, 4096], P(None, 'tensor')
- value_factor_gradient: float32 [64, 2048], P(None, 'tensor')
The draws below stay inside these ranges and needn't reach their ends.
Inputs may be any that keep to these rules, and one draw needn't show every extreme that they name: `lengths`: every sequence has at least one valid token and some sequence is full. `pairing`: entries 2k and 2k + 1 name the chosen and the rejected sequence of pair k; every sequence appears once.
All inputs are finite; a program needn't handle non-finite values.
Results may differ from the reference program's by a relative error of at most 0.0233.
The reference program's roundings to bfloat16 on the way count: a program that leaves them out, or rounds other values in their place, can miss the bound.
Values may be sent and summed in bfloat16 or wider, within the bound.
No kernel may reach another device: no remote copies, remote signals or barrier semaphores. Data moves between devices by JAX's collectives and lax.ppermute only.
A program may use at most 128 MiB of HBM per device.

```python
import jax
import jax.numpy as jnp
from jax import lax

MODEL_WIDTH = 4608
HQ = 32
KEY_VALUE_HEADS = 16
HEAD_SIZE = 128
ADAPTER_RANK = 64
SEQUENCE_SLOTS = 96
SEQUENCE_COUNT = 12
TOKEN_SLOTS = 1152
N_TENSOR = 8


def draw_lengths(key, part):
    first_key = jax.random.fold_in(key, 11)
    second_key = jax.random.fold_in(key, 12)
    lowest = max(1, SEQUENCE_SLOTS // 6)
    drawn = jax.random.randint(first_key, (SEQUENCE_COUNT,), lowest, SEQUENCE_SLOTS + 1)
    target_row = jax.random.randint(second_key, (), 0, SEQUENCE_COUNT)
    return jnp.where(jnp.arange(SEQUENCE_COUNT) == target_row, SEQUENCE_SLOTS, drawn).astype(jnp.int32)


def key_head_scales(scale_random_key, lowest, highest):
    uniform_sample = jax.random.uniform(scale_random_key, (KEY_VALUE_HEADS,), jnp.float32)
    spread_heads = jnp.exp(jnp.log(lowest) + uniform_sample * (jnp.log(highest) - jnp.log(lowest)))
    return (spread_heads[:, None] * jnp.ones((1, HEAD_SIZE), jnp.float32)).reshape(KEY_VALUE_HEADS * HEAD_SIZE)


def draw_w_key(key, part):
    scale_random_key = jax.random.fold_in(key, 21)
    entry_random_key = jax.random.fold_in(key, 22)
    spread_heads = key_head_scales(scale_random_key, 1.0, 8.0)
    table_entries = jax.random.truncated_normal(entry_random_key, -3.0, 3.0, (MODEL_WIDTH, KEY_VALUE_HEADS * HEAD_SIZE), jnp.float32)
    return (table_entries * spread_heads[None, :] * float(MODEL_WIDTH) ** (-0.5)).astype(jnp.bfloat16)


def steps_of(own_key, dims, cuts, least, high):
    level = 1.0
    for dim, parts in cuts:
        steps = jax.random.uniform(jax.random.fold_in(jax.random.fold_in(own_key, 6), dim), (parts,), jnp.float32, least / len(cuts), high / len(cuts))
        level = level * jnp.repeat(jnp.exp(steps), dims[dim] // parts).reshape((-1,) + (1,) * (len(dims) - 1 - dim))
    return level


def gaussian(key, extent, deviation, limit, split=(), kind=jnp.bfloat16):
    entries = deviation * jax.random.normal(key, extent, jnp.float32)
    if split:
        entries = entries * steps_of(key, extent, split, -0.22, 0.18)
    return jnp.clip(entries, -limit, limit).astype(kind)


def setup_inputs(seed: int = 0) -> dict:
    splits = jax.random.split(jax.random.key(seed), 16)
    return {
        "ref_hidden": gaussian(splits[0], (TOKEN_SLOTS, MODEL_WIDTH), 1.0, 6.0, ((0, 4), (1, 8))),
        "pol_hidden": gaussian(splits[1], (TOKEN_SLOTS, MODEL_WIDTH), 1.0, 6.0, ((0, 4), (1, 8))),
        "readout": gaussian(splits[2], (TOKEN_SLOTS, MODEL_WIDTH), 0.003, 0.019897461, ((0, 4), (1, 8))),
        "lengths": draw_lengths(jax.random.fold_in(splits[15], 71), 0),
        "pairing": jax.random.permutation(splits[4], SEQUENCE_COUNT).astype(jnp.int32),
        "pre_gain": jnp.clip(1.0 + 0.15 * jax.random.normal(splits[5], (MODEL_WIDTH,), jnp.float32), 0.25, 1.75),
        "post_gain": jnp.clip(1.0 + 0.15 * jax.random.normal(splits[6], (MODEL_WIDTH,), jnp.float32), 0.25, 1.75),
        "w_query": gaussian(splits[7], (MODEL_WIDTH, HQ * HEAD_SIZE), MODEL_WIDTH ** -0.5, 0.09375, ((0, 4), (1, 8))),
        "w_key": draw_w_key(jax.random.fold_in(splits[15], 71), 0),
        "value_projection": gaussian(splits[9], (MODEL_WIDTH, KEY_VALUE_HEADS * HEAD_SIZE), MODEL_WIDTH ** -0.5, 0.09375, ((0, 4), (1, 8))),
        "w_out": gaussian(splits[10], (MODEL_WIDTH, HQ * HEAD_SIZE), (HQ * HEAD_SIZE) ** -0.5, 0.09375, ((0, 4), (1, 8))),
        "a_query": gaussian(splits[11], (MODEL_WIDTH, ADAPTER_RANK), MODEL_WIDTH ** -0.5, 0.09375, ((0, 4),)),
        "a_value": gaussian(splits[12], (MODEL_WIDTH, ADAPTER_RANK), MODEL_WIDTH ** -0.5, 0.09375, ((0, 4),)),
        "query_second_factor": gaussian(splits[13], (ADAPTER_RANK, HQ * HEAD_SIZE), ADAPTER_RANK ** -0.5, 0.75, ((1, 8),)),
        "value_second_factor": gaussian(splits[14], (ADAPTER_RANK, KEY_VALUE_HEADS * HEAD_SIZE), ADAPTER_RANK ** -0.5, 0.75, ((1, 8),)),
    }


NORM_EPS = 1e-06
SOFT_CAP = 50.0
ADAPTER_SCALE = 0.5
DPO_BETA = 0.5
LOSS_SCALE = 256.0
ROPE_BASE = 10000.0

def query_scale():
    return float(MODEL_WIDTH // HQ) ** (-0.5)

def apply_rotation(value_rows, direction):
    length = value_rows.shape[1]
    head_depth = value_rows.shape[3]
    middle = head_depth // 2
    spacing = ROPE_BASE ** (-2.0 * jnp.arange(middle, dtype=jnp.float32) / head_depth)
    angles = jnp.arange(length, dtype=jnp.float32)[:, None] * spacing[None, :]
    cosine = jnp.cos(angles)[None, :, None, :]
    sine_part = direction * jnp.sin(angles)[None, :, None, :]
    leading = value_rows[..., :middle]
    trailing = value_rows[..., middle:]
    return jnp.concatenate([leading * cosine - trailing * sine_part, trailing * cosine + leading * sine_part], axis=-1)

def allowed_mask(lengths, length):
    places = jnp.arange(length)
    causal = places[None, :] <= places[:, None]
    living = places[None, :] < lengths[:, None]
    return causal[None, None, None, :, :] & living[:, None, None, None, :]

def attend(query_rows, rotated_keys, value_rows, lengths):
    seqs_here, length, q_heads, head_depth = query_rows.shape
    kv_heads = rotated_keys.shape[2]
    grouped_heads = query_rows.reshape(seqs_here, length, kv_heads, q_heads // kv_heads, head_depth)
    scores = jnp.einsum('sqkgd,spkd->skgqp', grouped_heads.astype(jnp.float32), rotated_keys.astype(jnp.float32)) * query_scale()
    capped = SOFT_CAP * jnp.tanh(scores / SOFT_CAP)
    allowed = allowed_mask(lengths, length)
    weights = jnp.where(allowed, jnp.exp(capped), 0.0)
    probabilities = weights / lax.optimization_barrier(jnp.sum(weights, axis=-1, keepdims=True))
    probs_low = probabilities.astype(jnp.bfloat16)
    mixed_out = jnp.einsum('skgqp,spkd->sqkgd', probs_low.astype(jnp.float32), value_rows.astype(jnp.float32))
    return (mixed_out.astype(jnp.bfloat16).reshape(seqs_here, length, q_heads, head_depth), probs_low, probabilities, capped)

def attend_back(grad_mixed, query_rows, rotated_keys, value_rows, probs_low, probabilities, capped):
    seqs_here, length, q_heads, head_depth = query_rows.shape
    kv_heads = rotated_keys.shape[2]
    shape_five = (seqs_here, length, kv_heads, q_heads // kv_heads, head_depth)
    grouped_heads = query_rows.reshape(shape_five).astype(jnp.float32)
    grad_grouped = grad_mixed.reshape(shape_five).astype(jnp.float32)
    grad_probs = jnp.einsum('sqkgd,spkd->skgqp', grad_grouped, value_rows.astype(jnp.float32))
    value_rows_gradient = jnp.einsum('skgqp,sqkgd->spkd', probs_low.astype(jnp.float32), grad_grouped)
    centered = grad_probs - lax.optimization_barrier(jnp.sum(grad_probs * probabilities, axis=-1, keepdims=True))
    grad_scores = (probabilities * centered * (1.0 - (capped / SOFT_CAP) ** 2) * query_scale()).astype(jnp.bfloat16)
    grad_scores = grad_scores.astype(jnp.float32)
    query_rows_gradient = jnp.einsum('skgqp,spkd->sqkgd', grad_scores, rotated_keys.astype(jnp.float32)).reshape(seqs_here, length, q_heads, head_depth)
    key_rows_gradient = jnp.einsum('skgqp,sqkgd->spkd', grad_scores, grouped_heads)
    return (query_rows_gradient, key_rows_gradient, value_rows_gradient)

def normalize(hidden, gain):
    wide_rows = hidden.astype(jnp.float32)
    pre_scale = lax.rsqrt(lax.optimization_barrier(jnp.sum(wide_rows * wide_rows, axis=1, keepdims=True)) / MODEL_WIDTH + NORM_EPS)
    return ((wide_rows * pre_scale * gain).astype(jnp.bfloat16), pre_scale)

def attention_layer(hidden, normed, lengths, post_gain, w_query, w_key, value_projection, w_out, adapters):
    query_rows = jnp.dot(normed, w_query, preferred_element_type=jnp.float32)
    keys_before_rotation = jnp.dot(normed, w_key, preferred_element_type=jnp.float32)
    value_rows = jnp.dot(normed, value_projection, preferred_element_type=jnp.float32)
    low_rank_update = None
    if adapters is not None:
        a_query, a_value, query_second_factor, value_second_factor = adapters
        low_rank_update = jnp.dot(normed, jnp.concatenate([a_query, a_value], axis=1), preferred_element_type=jnp.float32).astype(jnp.bfloat16)
        query_rows = query_rows + ADAPTER_SCALE * jnp.dot(low_rank_update[:, :ADAPTER_RANK], query_second_factor, preferred_element_type=jnp.float32)
        value_rows = value_rows + ADAPTER_SCALE * jnp.dot(low_rank_update[:, ADAPTER_RANK:], value_second_factor, preferred_element_type=jnp.float32)
    query_rows = apply_rotation(query_rows.reshape(SEQUENCE_COUNT, SEQUENCE_SLOTS, HQ, HEAD_SIZE), 1.0).astype(jnp.bfloat16)
    rotated_keys = apply_rotation(keys_before_rotation.reshape(SEQUENCE_COUNT, SEQUENCE_SLOTS, KEY_VALUE_HEADS, HEAD_SIZE), 1.0).astype(jnp.bfloat16)
    value_rows = value_rows.reshape(SEQUENCE_COUNT, SEQUENCE_SLOTS, KEY_VALUE_HEADS, HEAD_SIZE).astype(jnp.bfloat16)
    mixed_out, probs_low, probabilities, capped = attend(query_rows, rotated_keys, value_rows, lengths)
    flat_mixed = mixed_out.reshape(TOKEN_SLOTS, HQ * HEAD_SIZE)
    group_cols = HQ * HEAD_SIZE // N_TENSOR
    contract_cols = (((1,), (1,)), ((), ()))

    def add_group(index_g, running):
        start = (index_g * group_cols).astype(jnp.int32)
        columns = lax.dynamic_slice_in_dim(flat_mixed, start, group_cols, 1)
        w_columns = lax.dynamic_slice_in_dim(w_out, start, group_cols, 1)
        term_low = lax.dot_general(columns, w_columns, contract_cols, preferred_element_type=jnp.float32).astype(jnp.bfloat16)
        return running + lax.optimization_barrier(term_low).astype(jnp.float32)
    summed = lax.fori_loop(jnp.int32(0), jnp.int32(N_TENSOR), add_group, jnp.zeros((TOKEN_SLOTS, MODEL_WIDTH), jnp.float32))
    post_scale = lax.rsqrt(lax.optimization_barrier(jnp.sum(summed * summed, axis=1, keepdims=True)) / MODEL_WIDTH + NORM_EPS)
    result = hidden.astype(jnp.float32) + summed * post_scale * post_gain
    saved = (low_rank_update, query_rows, rotated_keys, value_rows, probs_low, probabilities, capped, summed, post_scale)
    return (result, saved)

def block_hook(grads, factor):
    grouped_heads = grads.astype(jnp.float32).reshape(TOKEN_SLOTS, N_TENSOR, -1)
    grouped_factors = factor.astype(jnp.float32).reshape(ADAPTER_RANK, N_TENSOR, -1)
    split_pieces = (ADAPTER_SCALE * jnp.einsum('fei,kei->fek', grouped_heads, grouped_factors)).astype(jnp.bfloat16)
    return lax.optimization_barrier(jnp.sum(lax.optimization_barrier(split_pieces).astype(jnp.float32), axis=1))

def reference(ref_hidden, pol_hidden, readout, lengths, pairing, pre_gain, post_gain, w_query, w_key, value_projection, w_out, a_query, a_value, query_second_factor, value_second_factor):
    ref_normed, ref_scale = normalize(ref_hidden, pre_gain)
    ref_result, ref_saved = attention_layer(ref_hidden, ref_normed, lengths, post_gain, w_query, w_key, value_projection, w_out, None)
    pol_normed, pol_scale = normalize(pol_hidden, pre_gain)
    pol_result, pol_saved = attention_layer(pol_hidden, pol_normed, lengths, post_gain, w_query, w_key, value_projection, w_out, (a_query, a_value, query_second_factor, value_second_factor))
    readout_wide = readout.astype(jnp.float32)
    living = (jnp.arange(SEQUENCE_SLOTS)[None, :] < lengths[:, None]).astype(jnp.float32)

    def sequence_score(result):
        return lax.optimization_barrier(jnp.sum(lax.optimization_barrier(jnp.sum(result * readout_wide, axis=1)).reshape(SEQUENCE_COUNT, SEQUENCE_SLOTS) * living, axis=1))
    ratios = sequence_score(pol_result) - sequence_score(ref_result)
    chosen = pairing[0::2]
    rejected = pairing[1::2]
    margins = DPO_BETA * (ratios[chosen] - ratios[rejected])
    dpo_loss = jnp.sum(jax.nn.softplus(-margins))
    pair_pull = DPO_BETA * LOSS_SCALE * jax.nn.sigmoid(-margins)
    coefficients = jnp.zeros((SEQUENCE_COUNT,), jnp.float32).at[chosen].add(-pair_pull).at[rejected].add(pair_pull)
    grad_result = (coefficients[:, None] * living).reshape(TOKEN_SLOTS, 1) * readout_wide
    low_rank_update, query_rows, rotated_keys, value_rows, probs_low, probabilities, capped, summed, post_scale = pol_saved
    post_dot = lax.optimization_barrier(jnp.sum(summed * post_gain * grad_result, axis=1, keepdims=True))
    grad_summed = post_scale * post_gain * grad_result - summed * post_scale ** 3 * post_dot / MODEL_WIDTH
    grad_wide = grad_summed.astype(jnp.bfloat16)
    grad_mixed = jnp.dot(grad_wide, w_out, preferred_element_type=jnp.float32).astype(jnp.bfloat16)
    grad_q_rot, rotated_key_gradient, value_head_gradient = attend_back(grad_mixed.reshape(SEQUENCE_COUNT, SEQUENCE_SLOTS, HQ, HEAD_SIZE), query_rows, rotated_keys, value_rows, probs_low, probabilities, capped)
    query_rows_gradient = apply_rotation(grad_q_rot, -1.0).reshape(TOKEN_SLOTS, HQ * HEAD_SIZE).astype(jnp.bfloat16)
    key_rows_gradient = apply_rotation(rotated_key_gradient, -1.0).reshape(TOKEN_SLOTS, KEY_VALUE_HEADS * HEAD_SIZE).astype(jnp.bfloat16)
    value_rows_gradient = value_head_gradient.reshape(TOKEN_SLOTS, KEY_VALUE_HEADS * HEAD_SIZE).astype(jnp.bfloat16)
    rows_contraction = (((0,), (0,)), ((), ()))
    contract_cols = (((1,), (1,)), ((), ()))
    query_factor_gradient = ADAPTER_SCALE * lax.dot_general(low_rank_update[:, :ADAPTER_RANK], query_rows_gradient, rows_contraction, preferred_element_type=jnp.float32)
    value_factor_gradient = ADAPTER_SCALE * lax.dot_general(low_rank_update[:, ADAPTER_RANK:], value_rows_gradient, rows_contraction, preferred_element_type=jnp.float32)
    adapter_grad = jnp.concatenate([block_hook(query_rows_gradient, query_second_factor), block_hook(value_rows_gradient, value_second_factor)], axis=1)
    grad_a = lax.dot_general(pol_normed.astype(jnp.float32), adapter_grad, rows_contraction, precision=lax.Precision.HIGHEST)
    a_both = jnp.concatenate([a_query, a_value], axis=1).astype(jnp.float32)
    grad_normed = lax.dot_general(query_rows_gradient, w_query, contract_cols, preferred_element_type=jnp.float32)
    grad_normed = grad_normed + lax.dot_general(key_rows_gradient, w_key, contract_cols, preferred_element_type=jnp.float32)
    grad_normed = grad_normed + lax.dot_general(value_rows_gradient, value_projection, contract_cols, preferred_element_type=jnp.float32)
    grad_normed = grad_normed + lax.dot_general(adapter_grad, a_both, contract_cols, precision=lax.Precision.HIGHEST)
    narrow = pol_hidden.astype(jnp.float32)
    pre_dot = lax.optimization_barrier(jnp.sum(narrow * pre_gain * grad_normed, axis=1, keepdims=True))
    grad_hidden = grad_result + pol_scale * pre_gain * grad_normed - narrow * pol_scale ** 3 * pre_dot / MODEL_WIDTH
    return (pol_result.astype(jnp.bfloat16), ref_result.astype(jnp.bfloat16), dpo_loss, grad_hidden.astype(jnp.bfloat16), grad_a, query_factor_gradient, value_factor_gradient)
```

```python
import jax
import jax.numpy as jnp
from jax import lax
from jax.sharding import PartitionSpec as P

MODEL_WIDTH = 4608
HQ = 32
HEAD_SIZE = 128


NORM_EPS = 1e-06
SOFT_CAP = 50.0
ADAPTER_SCALE = 0.5
DPO_BETA = 0.5
LOSS_SCALE = 256.0
ROPE_BASE = 10000.0


def query_scale():
    return float(MODEL_WIDTH // HQ) ** (-0.5)


def apply_rotation(value_rows, direction):
    length = value_rows.shape[1]
    head_depth = value_rows.shape[3]
    middle = head_depth // 2
    spacing = ROPE_BASE ** (-2.0 * jnp.arange(middle, dtype=jnp.float32) / head_depth)
    angles = jnp.arange(length, dtype=jnp.float32)[:, None] * spacing[None, :]
    cosine = jnp.cos(angles)[None, :, None, :]
    sine_part = direction * jnp.sin(angles)[None, :, None, :]
    leading = value_rows[..., :middle]
    trailing = value_rows[..., middle:]
    return jnp.concatenate(
        [leading * cosine - trailing * sine_part, trailing * cosine + leading * sine_part], axis=-1
    )


def allowed_mask(lengths, length):
    places = jnp.arange(length)
    causal = places[None, :] <= places[:, None]
    living = places[None, :] < lengths[:, None]
    return causal[None, None, None, :, :] & living[:, None, None, None, :]


def attend(query_rows, rotated_keys, value_rows, lengths):
    seqs_here, length, q_heads, head_depth = query_rows.shape
    kv_heads = rotated_keys.shape[2]
    grouped_heads = query_rows.reshape(seqs_here, length, kv_heads, q_heads // kv_heads, head_depth)
    scores = (
        jnp.einsum(
            "sqkgd,spkd->skgqp", grouped_heads, rotated_keys, preferred_element_type=jnp.float32
        )
        * query_scale()
    )
    capped = SOFT_CAP * jnp.tanh(scores / SOFT_CAP)
    allowed = allowed_mask(lengths, length)
    weights = jnp.where(allowed, jnp.exp(capped), 0.0)
    probabilities = weights / jnp.sum(weights, axis=-1, keepdims=True)
    probs_low = probabilities.astype(jnp.bfloat16)
    mixed_out = jnp.einsum(
        "skgqp,spkd->sqkgd", probs_low, value_rows, preferred_element_type=jnp.float32
    )
    return (
        mixed_out.astype(jnp.bfloat16).reshape(seqs_here, length, q_heads, head_depth),
        probs_low,
        probabilities,
        capped,
    )


def attend_back(grad_mixed, query_rows, rotated_keys, value_rows, probs_low, probabilities, capped):
    seqs_here, length, q_heads, head_depth = query_rows.shape
    kv_heads = rotated_keys.shape[2]
    shape_five = (seqs_here, length, kv_heads, q_heads // kv_heads, head_depth)
    grouped_heads = query_rows.reshape(shape_five)
    grad_grouped = grad_mixed.reshape(shape_five)
    grad_probs = jnp.einsum(
        "sqkgd,spkd->skgqp", grad_grouped, value_rows, preferred_element_type=jnp.float32
    )
    value_rows_gradient = jnp.einsum(
        "skgqp,sqkgd->spkd", probs_low, grad_grouped, preferred_element_type=jnp.float32
    )
    centered = grad_probs - jnp.sum(grad_probs * probabilities, axis=-1, keepdims=True)
    grad_scores = (
        probabilities * centered * (1.0 - (capped / SOFT_CAP) ** 2) * query_scale()
    ).astype(jnp.bfloat16)
    query_rows_gradient = jnp.einsum(
        "skgqp,spkd->sqkgd", grad_scores, rotated_keys, preferred_element_type=jnp.float32
    ).reshape(seqs_here, length, q_heads, head_depth)
    key_rows_gradient = jnp.einsum(
        "skgqp,sqkgd->spkd", grad_scores, grouped_heads, preferred_element_type=jnp.float32
    )
    return (query_rows_gradient, key_rows_gradient, value_rows_gradient)


def minor_of(size):
    minor = 2
    while size // minor > 2 * minor:
        minor *= 2
    return minor if size % minor == 0 else 1


def shift_major(x, axis, minor, k):
    size = lax.axis_size(axis)
    return lax.ppermute(x, axis, [(i, (i + k * minor) % size) for i in range(size)])


def shift_minor(x, axis, minor, k):
    size = lax.axis_size(axis)
    return lax.ppermute(
        x, axis, [(i, i // minor * minor + (i % minor + k) % minor) for i in range(size)]
    )


def gather_parts(x, axis, minor):
    size = lax.axis_size(axis)
    major = size // minor
    me = lax.axis_index(axis)
    column = [x] + [shift_major(x, axis, minor, k) for k in range(1, major)]
    parts = []
    for m in range(minor):
        for k in range(major):
            rank = ((me // minor - k) % major) * minor + (me % minor - m) % minor
            parts.append((rank, column[k] if m == 0 else shift_minor(column[k], axis, minor, m)))
    return parts


def gather_ranks(x, axis, minor):
    whole = jnp.zeros((lax.axis_size(axis),) + x.shape, x.dtype)
    for rank, part in gather_parts(x, axis, minor):
        whole = lax.dynamic_update_index_in_dim(whole, part, rank, 0)
    return whole


def sum_ranks(x, axis, minor):
    return jnp.sum(gather_ranks(x, axis, minor).astype(jnp.float32), axis=0)


def scatter_sum(chunk_of, axis, minor):
    size = lax.axis_size(axis)
    major = size // minor
    me = lax.axis_index(axis)
    high, low = me // minor, me % minor
    total = None
    for k in list(range(1, major)) + [0]:
        row = ((high + k) % major) * minor
        value = chunk_of(row + low).astype(jnp.float32)
        for m in range(1, minor):
            sent = chunk_of(row + (low + m) % minor)
            value = value + shift_minor(sent, axis, minor, m).astype(jnp.float32)
        if k:
            value = shift_major(value.astype(jnp.bfloat16), axis, minor, k).astype(jnp.float32)
        total = value if total is None else total + value
    return total


def normalize(hidden, gain_chunks, minor):
    chunks = gather_ranks(hidden, "tensor", minor).astype(jnp.float32)
    full_width = gain_chunks.shape[0] * gain_chunks.shape[1]
    squares = jnp.sum(jnp.sum(chunks * chunks, axis=2), axis=0)[:, None]
    pre_scale = lax.rsqrt(squares / full_width + NORM_EPS)
    normed = (chunks * pre_scale[None] * gain_chunks[:, None, :]).astype(jnp.bfloat16)
    return (normed, pre_scale)


def take(chunks, index):
    return lax.dynamic_index_in_dim(chunks, index, 0, keepdims=False)


def rows_product(chunks, parts):
    width = chunks.shape[2]
    total = None
    for rank, part in parts:
        per = part.shape[0] // width
        for i in range(per):
            term = jnp.dot(
                take(chunks, rank * per + i),
                part[i * width : (i + 1) * width],
                preferred_element_type=jnp.float32,
            )
            total = term if total is None else total + term
    return total


def columns_product(rows, parts, width):
    tok_rows = rows.shape[0]
    per = parts[0][1].shape[0] // width
    pieces = None
    for rank, part in parts:
        for i in range(per):
            piece = lax.dot_general(
                rows,
                part[i * width : (i + 1) * width],
                (((1,), (1,)), ((), ())),
                preferred_element_type=jnp.float32,
            ).astype(jnp.bfloat16)
            if pieces is None:
                pieces = jnp.zeros((len(parts) * per, tok_rows, width), jnp.bfloat16)
            pieces = lax.dynamic_update_index_in_dim(pieces, piece, rank * per + i, 0)
    return lambda c: take(pieces, c)


def attention_layer(normed, in_parts, out_parts, adapters, widths, lengths, minor):
    tok_rows, width = normed.shape[1:]
    seqs_here = lengths.shape[0]
    length = tok_rows // seqs_here
    q_cols, k_cols, v_cols, rank_size = widths
    projected = rows_product(normed, in_parts)
    query_rows = projected[:, :q_cols]
    keys_before_rotation = projected[:, q_cols : q_cols + k_cols]
    value_rows = projected[:, q_cols + k_cols : q_cols + k_cols + v_cols]
    low_rank_update = None
    if adapters is not None:
        query_second_factor, value_second_factor = adapters
        low_rank_update = projected[:, q_cols + k_cols + v_cols :].astype(jnp.bfloat16)
        query_rows = query_rows + ADAPTER_SCALE * jnp.dot(
            low_rank_update[:, :rank_size], query_second_factor, preferred_element_type=jnp.float32
        )
        value_rows = value_rows + ADAPTER_SCALE * jnp.dot(
            low_rank_update[:, rank_size:], value_second_factor, preferred_element_type=jnp.float32
        )
    q_heads = q_cols // HEAD_SIZE
    kv_heads = k_cols // HEAD_SIZE
    query_rows = apply_rotation(
        query_rows.reshape(seqs_here, length, q_heads, HEAD_SIZE), 1.0
    ).astype(jnp.bfloat16)
    rotated_keys = apply_rotation(
        keys_before_rotation.reshape(seqs_here, length, kv_heads, HEAD_SIZE), 1.0
    ).astype(jnp.bfloat16)
    value_rows = value_rows.reshape(seqs_here, length, kv_heads, HEAD_SIZE).astype(jnp.bfloat16)
    mixed_out, probs_low, probabilities, capped = attend(
        query_rows, rotated_keys, value_rows, lengths
    )
    terms = columns_product(mixed_out.reshape(tok_rows, q_cols), out_parts, width)
    summed = scatter_sum(terms, "tensor", minor)
    saved = (
        low_rank_update,
        query_rows,
        rotated_keys,
        value_rows,
        probs_low,
        probabilities,
        capped,
    )
    return (summed, saved)


def body(
    ref_hidden,
    pol_hidden,
    readout,
    lengths,
    pairing,
    pre_gain,
    post_gain,
    w_query,
    w_key,
    value_projection,
    w_out,
    a_query,
    a_value,
    query_second_factor,
    value_second_factor,
):
    tok_rows, part_width = pol_hidden.shape
    seqs_here = lengths.shape[0]
    length = tok_rows // seqs_here
    tensor_rank = lax.axis_index("tensor")
    data_rank = lax.axis_index("dp")
    all_seqs = seqs_here * lax.axis_size("dp")
    full_width = part_width * lax.axis_size("tensor")
    pre_local = lax.dynamic_slice_in_dim(pre_gain, tensor_rank * part_width, part_width)
    post_local = lax.dynamic_slice_in_dim(post_gain, tensor_rank * part_width, part_width)
    data_size, tensor_size = lax.axis_size("dp"), lax.axis_size("tensor")
    minor = minor_of(tensor_size)
    data_minor = 2 if data_size % 2 == 0 else 1
    gain_chunks = pre_gain.reshape(tensor_size, part_width)
    q_cols, k_cols, v_cols = w_query.shape[1], w_key.shape[1], value_projection.shape[1]
    rank_size = a_query.shape[1]
    widths = (q_cols, k_cols, v_cols, rank_size)
    in_parts = gather_parts(
        jnp.concatenate([w_query, w_key, value_projection, a_query, a_value], axis=1),
        "dp",
        data_minor,
    )
    out_parts = gather_parts(w_out, "dp", data_minor)
    ref_normed, ref_scale = normalize(ref_hidden, gain_chunks, minor)
    pol_normed, pol_scale = normalize(pol_hidden, gain_chunks, minor)
    ref_summed, _ = attention_layer(
        ref_normed, in_parts, out_parts, None, widths, lengths, minor
    )
    summed, pol_saved = attention_layer(
        pol_normed,
        in_parts,
        out_parts,
        (query_second_factor, value_second_factor),
        widths,
        lengths,
        minor,
    )
    readout_wide = readout.astype(jnp.float32)
    living = (jnp.arange(length)[None, :] < lengths[:, None]).astype(jnp.float32)

    def token_sums(hidden, total):
        return jnp.stack(
            [
                jnp.sum(total * total, axis=1),
                jnp.sum(total * post_local * readout_wide, axis=1),
                jnp.sum(hidden.astype(jnp.float32) * readout_wide, axis=1),
            ]
        )

    ref_sums = sum_ranks(token_sums(ref_hidden, ref_summed), "tensor", minor)
    pol_sums = sum_ranks(token_sums(pol_hidden, summed), "tensor", minor)
    ref_post = lax.rsqrt(ref_sums[0] / full_width + NORM_EPS)
    pol_post = lax.rsqrt(pol_sums[0] / full_width + NORM_EPS)
    post_scale = pol_post[:, None]
    ref_result = ref_hidden.astype(jnp.float32) + ref_summed * ref_post[:, None] * post_local
    pol_result = pol_hidden.astype(jnp.float32) + summed * post_scale * post_local

    def sequence_score(sums, scale):
        return jnp.sum((sums[2] + scale * sums[1]).reshape(seqs_here, length) * living, axis=1)

    scores_here = jnp.stack([sequence_score(ref_sums, ref_post), sequence_score(pol_sums, pol_post)])
    offset = data_rank * seqs_here
    scores = jnp.transpose(gather_ranks(scores_here, "dp", data_minor), (1, 0, 2)).reshape(2, all_seqs)
    ratios = scores[1] - scores[0]
    chooser = (pairing[:, None] == jnp.arange(all_seqs)[None, :]).astype(jnp.float32)
    picked = jnp.dot(chooser, ratios, precision=lax.Precision.HIGHEST).reshape(-1, 2)
    margins = DPO_BETA * (picked[:, 0] - picked[:, 1])
    dpo_loss = jnp.sum(jax.nn.softplus(-margins))
    pair_pull = DPO_BETA * LOSS_SCALE * jax.nn.sigmoid(-margins)
    signed = jnp.stack([-pair_pull, pair_pull], axis=1).reshape(-1)
    coefficients = jnp.dot(signed, chooser, precision=lax.Precision.HIGHEST)
    local_coef = lax.dynamic_slice_in_dim(coefficients, offset, seqs_here)
    grad_result = (local_coef[:, None] * living).reshape(tok_rows, 1) * readout_wide
    (
        low_rank_update,
        query_rows,
        rotated_keys,
        value_rows,
        probs_low,
        probabilities,
        capped,
    ) = pol_saved
    token_coef = (local_coef[:, None] * living).reshape(tok_rows)
    post_dot = token_coef * pol_sums[1]
    grad_summed = (
        post_scale * post_local * grad_result
        - summed * post_scale**3 * post_dot[:, None] / full_width
    )
    grad_chunks = gather_ranks(grad_summed.astype(jnp.bfloat16), "tensor", minor)
    grad_mixed = rows_product(grad_chunks, out_parts).astype(jnp.bfloat16)
    q_heads = query_rows.shape[2]
    grad_q_rot, rotated_key_gradient, value_head_gradient = attend_back(
        grad_mixed.reshape(seqs_here, length, q_heads, HEAD_SIZE),
        query_rows,
        rotated_keys,
        value_rows,
        probs_low,
        probabilities,
        capped,
    )
    query_rows_gradient = (
        apply_rotation(grad_q_rot, -1.0).reshape(tok_rows, -1).astype(jnp.bfloat16)
    )
    key_rows_gradient = (
        apply_rotation(rotated_key_gradient, -1.0).reshape(tok_rows, -1).astype(jnp.bfloat16)
    )
    value_rows_gradient = value_head_gradient.reshape(tok_rows, -1).astype(jnp.bfloat16)
    rows_contraction = (((0,), (0,)), ((), ()))
    contract_cols = (((1,), (1,)), ((), ()))
    query_adapter_term = ADAPTER_SCALE * lax.dot_general(
        low_rank_update[:, :rank_size],
        query_rows_gradient,
        rows_contraction,
        preferred_element_type=jnp.float32,
    )
    value_adapter_term = ADAPTER_SCALE * lax.dot_general(
        low_rank_update[:, rank_size:],
        value_rows_gradient,
        rows_contraction,
        preferred_element_type=jnp.float32,
    )
    factor_gradient = sum_ranks(
        jnp.concatenate([query_adapter_term, value_adapter_term], axis=1).astype(jnp.bfloat16),
        "dp",
        data_minor,
    )
    query_factor_gradient = factor_gradient[:, :q_cols]
    value_factor_gradient = factor_gradient[:, q_cols:]
    adapter_grad = jnp.concatenate(
        [
            ADAPTER_SCALE
            * lax.dot_general(
                query_rows_gradient,
                query_second_factor,
                contract_cols,
                preferred_element_type=jnp.float32,
            ),
            ADAPTER_SCALE
            * lax.dot_general(
                value_rows_gradient,
                value_second_factor,
                contract_cols,
                preferred_element_type=jnp.float32,
            ),
        ],
        axis=1,
    ).astype(jnp.bfloat16)
    input_rows = jnp.concatenate(
        [query_rows_gradient, key_rows_gradient, value_rows_gradient, adapter_grad], axis=1
    )
    grad_normed = scatter_sum(
        columns_product(input_rows, in_parts, part_width), "tensor", minor
    )
    hook = sum_ranks(adapter_grad, "tensor", minor).astype(jnp.bfloat16)
    adapter_term = jnp.stack(
        [
            lax.dot_general(
                pol_normed[c], hook, rows_contraction, preferred_element_type=jnp.float32
            ).astype(jnp.bfloat16)
            for c in range(tensor_size)
        ]
    ).reshape(data_size, full_width // data_size, 2 * rank_size)
    grad_a = scatter_sum(lambda d: take(adapter_term, d), "dp", data_minor)
    narrow = pol_hidden.astype(jnp.float32)
    pre_dot = sum_ranks(jnp.sum(narrow * pre_local * grad_normed, axis=1), "tensor", minor)
    grad_hidden = (
        grad_result
        + pol_scale * pre_local * grad_normed
        - narrow * pol_scale**3 * pre_dot[:, None] / full_width
    )
    return (
        pol_result.astype(jnp.bfloat16),
        ref_result.astype(jnp.bfloat16),
        dpo_loss,
        grad_hidden.astype(jnp.bfloat16),
        grad_a,
        query_factor_gradient,
        value_factor_gradient,
    )


def solution(mesh):
    placed = (
        P("dp", "tensor"),
        P("dp", "tensor"),
        P("dp", "tensor"),
        P("dp"),
        P(),
        P(),
        P(),
        P("dp", "tensor"),
        P("dp", "tensor"),
        P("dp", "tensor"),
        P("dp", "tensor"),
        P("dp", None),
        P("dp", None),
        P(None, "tensor"),
        P(None, "tensor"),
    )
    return jax.shard_map(
        body,
        mesh=mesh,
        in_specs=placed,
        out_specs=(
            P("dp", "tensor"),
            P("dp", "tensor"),
            P(),
            P("dp", "tensor"),
            P("dp", None),
            P(None, "tensor"),
            P(None, "tensor"),
        ),
        check_vma=False,
    )
```

```python
import jax
import jax.numpy as jnp
from jax import lax
from jax.sharding import PartitionSpec as P

MODEL_WIDTH = 4608
HQ = 32
HEAD_SIZE = 128


NORM_EPS = 1e-06
SOFT_CAP = 50.0
ADAPTER_SCALE = 0.5
DPO_BETA = 0.5
LOSS_SCALE = 256.0
ROPE_BASE = 10000.0


def query_scale():
    return float(MODEL_WIDTH // HQ) ** (-0.5)


def apply_rotation(value_rows, direction):
    length = value_rows.shape[1]
    head_depth = value_rows.shape[3]
    middle = head_depth // 2
    spacing = ROPE_BASE ** (-2.0 * jnp.arange(middle, dtype=jnp.float32) / head_depth)
    angles = jnp.arange(length, dtype=jnp.float32)[:, None] * spacing[None, :]
    cosine = jnp.cos(angles)[None, :, None, :]
    sine_part = direction * jnp.sin(angles)[None, :, None, :]
    leading = value_rows[..., :middle]
    trailing = value_rows[..., middle:]
    return jnp.concatenate(
        [leading * cosine - trailing * sine_part, trailing * cosine + leading * sine_part], axis=-1
    )


def allowed_mask(lengths, length):
    places = jnp.arange(length)
    causal = places[None, :] <= places[:, None]
    living = places[None, :] < lengths[:, None]
    return causal[None, None, None, :, :] & living[:, None, None, None, :]


def attend(query_rows, rotated_keys, value_rows, lengths):
    seqs_here, length, q_heads, head_depth = query_rows.shape
    kv_heads = rotated_keys.shape[2]
    grouped_heads = query_rows.reshape(seqs_here, length, kv_heads, q_heads // kv_heads, head_depth)
    scores = (
        jnp.einsum(
            "sqkgd,spkd->skgqp", grouped_heads, rotated_keys, preferred_element_type=jnp.float32
        )
        * query_scale()
    )
    capped = SOFT_CAP * jnp.tanh(scores / SOFT_CAP)
    allowed = allowed_mask(lengths, length)
    weights = jnp.where(allowed, jnp.exp(capped), 0.0)
    probabilities = weights / jnp.sum(weights, axis=-1, keepdims=True)
    probs_low = probabilities.astype(jnp.bfloat16)
    mixed_out = jnp.einsum(
        "skgqp,spkd->skgqd", probs_low, value_rows, preferred_element_type=jnp.float32
    ).astype(jnp.bfloat16)
    group = q_heads // kv_heads
    heads = [
        mixed_out[:, j // group, j % group].reshape(seqs_here * length, head_depth)
        for j in range(q_heads)
    ]
    return (
        jnp.concatenate(heads, axis=1),
        probs_low,
        probabilities,
        capped,
    )


def attend_back(grad_mixed, query_rows, rotated_keys, value_rows, probs_low, probabilities, capped):
    seqs_here, length, q_heads, head_depth = query_rows.shape
    kv_heads = rotated_keys.shape[2]
    shape_five = (seqs_here, length, kv_heads, q_heads // kv_heads, head_depth)
    grouped_heads = query_rows.reshape(shape_five)
    grad_grouped = grad_mixed.reshape(shape_five)
    grad_probs = jnp.einsum(
        "sqkgd,spkd->skgqp", grad_grouped, value_rows, preferred_element_type=jnp.float32
    )
    value_rows_gradient = jnp.einsum(
        "skgqp,sqkgd->spkd", probs_low, grad_grouped, preferred_element_type=jnp.float32
    )
    centered = grad_probs - jnp.sum(grad_probs * probabilities, axis=-1, keepdims=True)
    grad_scores = (
        probabilities * centered * (1.0 - (capped / SOFT_CAP) ** 2) * query_scale()
    ).astype(jnp.bfloat16)
    query_rows_gradient = jnp.einsum(
        "skgqp,spkd->sqkgd", grad_scores, rotated_keys, preferred_element_type=jnp.float32
    ).reshape(seqs_here, length, q_heads, head_depth)
    key_rows_gradient = jnp.einsum(
        "skgqp,sqkgd->spkd", grad_scores, grouped_heads, preferred_element_type=jnp.float32
    )
    return (query_rows_gradient, key_rows_gradient, value_rows_gradient)


def minor_of(size):
    minor = 2
    while size // minor > 2 * minor:
        minor *= 2
    return minor if size % minor == 0 else 1


def shift_major(x, axis, minor, k):
    size = lax.axis_size(axis)
    return lax.ppermute(x, axis, [(i, (i + k * minor) % size) for i in range(size)])


def shift_minor(x, axis, minor, k):
    size = lax.axis_size(axis)
    return lax.ppermute(
        x, axis, [(i, i // minor * minor + (i % minor + k) % minor) for i in range(size)]
    )


def gather_parts(x, axis, minor):
    size = lax.axis_size(axis)
    major = size // minor
    me = lax.axis_index(axis)
    column = [x] + [shift_major(x, axis, minor, k) for k in range(1, major)]
    parts = []
    for m in range(minor):
        for k in range(major):
            rank = ((me // minor - k) % major) * minor + (me % minor - m) % minor
            parts.append((rank, column[k] if m == 0 else shift_minor(column[k], axis, minor, m)))
    return parts


def gather_ranks(x, axis, minor):
    whole = jnp.zeros((lax.axis_size(axis),) + x.shape, x.dtype)
    for rank, part in gather_parts(x, axis, minor):
        whole = lax.dynamic_update_index_in_dim(whole, part, rank, 0)
    return whole


def sum_ranks(x, axis, minor):
    return jnp.sum(gather_ranks(x, axis, minor).astype(jnp.float32), axis=0)


def scatter_sum(chunk_of, axis, minor):
    size = lax.axis_size(axis)
    major = size // minor
    me = lax.axis_index(axis)
    high, low = me // minor, me % minor
    total = None
    for k in list(range(1, major)) + [0]:
        row = ((high + k) % major) * minor
        value = chunk_of(row + low).astype(jnp.float32)
        for m in range(1, minor):
            sent = chunk_of(row + (low + m) % minor)
            value = value + shift_minor(sent, axis, minor, m).astype(jnp.float32)
        if k:
            value = shift_major(value.astype(jnp.bfloat16), axis, minor, k).astype(jnp.float32)
        total = value if total is None else total + value
    return total


def normalize(hidden, gain_chunks, minor):
    chunks = gather_ranks(hidden, "tensor", minor).astype(jnp.float32)
    full_width = gain_chunks.shape[0] * gain_chunks.shape[1]
    squares = jnp.sum(jnp.sum(chunks * chunks, axis=2), axis=0)[:, None]
    pre_scale = lax.rsqrt(squares / full_width + NORM_EPS)
    normed = (chunks * pre_scale[None] * gain_chunks[:, None, :]).astype(jnp.bfloat16)
    return (normed, pre_scale)


def take(chunks, index):
    return lax.dynamic_index_in_dim(chunks, index, 0, keepdims=False)


def rows_product(chunks, parts):
    width = chunks.shape[2]
    total = None
    for rank, part in parts:
        per = part.shape[0] // width
        for i in range(per):
            term = jnp.dot(
                take(chunks, rank * per + i),
                part[i * width : (i + 1) * width],
                preferred_element_type=jnp.float32,
            )
            total = term if total is None else total + term
    return total


def columns_product(rows, parts, width):
    tok_rows = rows.shape[0]
    per = parts[0][1].shape[0] // width
    pieces = None
    for rank, part in parts:
        for i in range(per):
            piece = lax.dot_general(
                rows,
                part[i * width : (i + 1) * width],
                (((1,), (1,)), ((), ())),
                preferred_element_type=jnp.float32,
            ).astype(jnp.bfloat16)
            if pieces is None:
                pieces = jnp.zeros((len(parts) * per, tok_rows, width), jnp.bfloat16)
            pieces = lax.dynamic_update_index_in_dim(pieces, piece, rank * per + i, 0)
    return lambda c: take(pieces, c)


def attention_layer(normed, in_parts, out_parts, adapters, widths, lengths, minor):
    tok_rows, width = normed.shape[1:]
    seqs_here = lengths.shape[0]
    length = tok_rows // seqs_here
    q_cols, k_cols, v_cols, rank_size = widths
    projected = rows_product(normed, in_parts)
    query_rows = projected[:, :q_cols]
    keys_before_rotation = projected[:, q_cols : q_cols + k_cols]
    value_rows = projected[:, q_cols + k_cols : q_cols + k_cols + v_cols]
    low_rank_update = None
    if adapters is not None:
        query_second_factor, value_second_factor = adapters
        low_rank_update = projected[:, q_cols + k_cols + v_cols :].astype(jnp.bfloat16)
        query_rows = query_rows + ADAPTER_SCALE * jnp.dot(
            low_rank_update[:, :rank_size], query_second_factor, preferred_element_type=jnp.float32
        )
        value_rows = value_rows + ADAPTER_SCALE * jnp.dot(
            low_rank_update[:, rank_size:], value_second_factor, preferred_element_type=jnp.float32
        )
    q_heads = q_cols // HEAD_SIZE
    kv_heads = k_cols // HEAD_SIZE
    query_rows = apply_rotation(
        query_rows.reshape(seqs_here, length, q_heads, HEAD_SIZE), 1.0
    ).astype(jnp.bfloat16)
    rotated_keys = apply_rotation(
        keys_before_rotation.reshape(seqs_here, length, kv_heads, HEAD_SIZE), 1.0
    ).astype(jnp.bfloat16)
    value_rows = value_rows.reshape(seqs_here, length, kv_heads, HEAD_SIZE).astype(jnp.bfloat16)
    mixed_out, probs_low, probabilities, capped = attend(
        query_rows, rotated_keys, value_rows, lengths
    )
    terms = columns_product(mixed_out, out_parts, width)
    summed = scatter_sum(terms, "tensor", minor)
    saved = (
        low_rank_update,
        query_rows,
        rotated_keys,
        value_rows,
        probs_low,
        probabilities,
        capped,
    )
    return (summed, saved)


def body(
    ref_hidden,
    pol_hidden,
    readout,
    lengths,
    pairing,
    pre_gain,
    post_gain,
    w_query,
    w_key,
    value_projection,
    w_out,
    a_query,
    a_value,
    query_second_factor,
    value_second_factor,
):
    tok_rows, part_width = pol_hidden.shape
    seqs_here = lengths.shape[0]
    length = tok_rows // seqs_here
    tensor_rank = lax.axis_index("tensor")
    data_rank = lax.axis_index("dp")
    all_seqs = seqs_here * lax.axis_size("dp")
    full_width = part_width * lax.axis_size("tensor")
    pre_local = lax.dynamic_slice_in_dim(pre_gain, tensor_rank * part_width, part_width)
    post_local = lax.dynamic_slice_in_dim(post_gain, tensor_rank * part_width, part_width)
    data_size, tensor_size = lax.axis_size("dp"), lax.axis_size("tensor")
    minor = minor_of(tensor_size)
    data_minor = 2 if data_size % 2 == 0 else 1
    gain_chunks = pre_gain.reshape(tensor_size, part_width)
    q_cols, k_cols, v_cols = w_query.shape[1], w_key.shape[1], value_projection.shape[1]
    rank_size = a_query.shape[1]
    widths = (q_cols, k_cols, v_cols, rank_size)
    in_parts = gather_parts(
        jnp.concatenate([w_query, w_key, value_projection, a_query, a_value], axis=1),
        "dp",
        data_minor,
    )
    out_parts = gather_parts(w_out, "dp", data_minor)
    ref_normed, ref_scale = normalize(ref_hidden, gain_chunks, minor)
    pol_normed, pol_scale = normalize(pol_hidden, gain_chunks, minor)
    ref_summed, _ = attention_layer(
        ref_normed, in_parts, out_parts, None, widths, lengths, minor
    )
    summed, pol_saved = attention_layer(
        pol_normed,
        in_parts,
        out_parts,
        (query_second_factor, value_second_factor),
        widths,
        lengths,
        minor,
    )
    readout_wide = readout.astype(jnp.float32)
    living = (jnp.arange(length)[None, :] < lengths[:, None]).astype(jnp.float32)

    def token_sums(hidden, total):
        return jnp.stack(
            [
                jnp.sum(total * total, axis=1),
                jnp.sum(total * post_local * readout_wide, axis=1),
                jnp.sum(hidden.astype(jnp.float32) * readout_wide, axis=1),
            ]
        )

    ref_sums = sum_ranks(token_sums(ref_hidden, ref_summed), "tensor", minor)
    pol_sums = sum_ranks(token_sums(pol_hidden, summed), "tensor", minor)
    ref_post = lax.rsqrt(ref_sums[0] / full_width + NORM_EPS)
    pol_post = lax.rsqrt(pol_sums[0] / full_width + NORM_EPS)
    post_scale = pol_post[:, None]
    ref_result = ref_hidden.astype(jnp.float32) + ref_summed * ref_post[:, None] * post_local
    pol_result = pol_hidden.astype(jnp.float32) + summed * post_scale * post_local

    def sequence_score(sums, scale):
        return jnp.sum((sums[2] + scale * sums[1]).reshape(seqs_here, length) * living, axis=1)

    scores_here = jnp.stack([sequence_score(ref_sums, ref_post), sequence_score(pol_sums, pol_post)])
    offset = data_rank * seqs_here
    scores = jnp.transpose(gather_ranks(scores_here, "dp", data_minor), (1, 0, 2)).reshape(2, all_seqs)
    ratios = scores[1] - scores[0]
    chooser = (pairing[:, None] == jnp.arange(all_seqs)[None, :]).astype(jnp.float32)
    picked = jnp.dot(chooser, ratios, precision=lax.Precision.HIGHEST).reshape(-1, 2)
    margins = DPO_BETA * (picked[:, 0] - picked[:, 1])
    dpo_loss = jnp.sum(jax.nn.softplus(-margins))
    pair_pull = DPO_BETA * LOSS_SCALE * jax.nn.sigmoid(-margins)
    signed = jnp.stack([-pair_pull, pair_pull], axis=1).reshape(-1)
    coefficients = jnp.dot(signed, chooser, precision=lax.Precision.HIGHEST)
    local_coef = lax.dynamic_slice_in_dim(coefficients, offset, seqs_here)
    grad_result = (local_coef[:, None] * living).reshape(tok_rows, 1) * readout_wide
    (
        low_rank_update,
        query_rows,
        rotated_keys,
        value_rows,
        probs_low,
        probabilities,
        capped,
    ) = pol_saved
    token_coef = (local_coef[:, None] * living).reshape(tok_rows)
    post_dot = token_coef * pol_sums[1]
    grad_summed = (
        post_scale * post_local * grad_result
        - summed * post_scale**3 * post_dot[:, None] / full_width
    )
    grad_chunks = gather_ranks(grad_summed.astype(jnp.bfloat16), "tensor", minor)
    grad_mixed = rows_product(grad_chunks, out_parts).astype(jnp.bfloat16)
    q_heads = query_rows.shape[2]
    grad_q_rot, rotated_key_gradient, value_head_gradient = attend_back(
        grad_mixed.reshape(seqs_here, length, q_heads, HEAD_SIZE),
        query_rows,
        rotated_keys,
        value_rows,
        probs_low,
        probabilities,
        capped,
    )
    query_rows_gradient = (
        apply_rotation(grad_q_rot, -1.0).reshape(tok_rows, -1).astype(jnp.bfloat16)
    )
    key_rows_gradient = (
        apply_rotation(rotated_key_gradient, -1.0).reshape(tok_rows, -1).astype(jnp.bfloat16)
    )
    value_rows_gradient = value_head_gradient.reshape(tok_rows, -1).astype(jnp.bfloat16)
    rows_contraction = (((0,), (0,)), ((), ()))
    contract_cols = (((1,), (1,)), ((), ()))
    query_adapter_term = ADAPTER_SCALE * lax.dot_general(
        low_rank_update[:, :rank_size],
        query_rows_gradient,
        rows_contraction,
        preferred_element_type=jnp.float32,
    )
    value_adapter_term = ADAPTER_SCALE * lax.dot_general(
        low_rank_update[:, rank_size:],
        value_rows_gradient,
        rows_contraction,
        preferred_element_type=jnp.float32,
    )
    factor_gradient = sum_ranks(
        jnp.concatenate([query_adapter_term, value_adapter_term], axis=1).astype(jnp.bfloat16),
        "dp",
        data_minor,
    )
    query_factor_gradient = factor_gradient[:, :q_cols]
    value_factor_gradient = factor_gradient[:, q_cols:]
    adapter_grad = jnp.concatenate(
        [
            ADAPTER_SCALE
            * lax.dot_general(
                query_rows_gradient,
                query_second_factor,
                contract_cols,
                preferred_element_type=jnp.float32,
            ),
            ADAPTER_SCALE
            * lax.dot_general(
                value_rows_gradient,
                value_second_factor,
                contract_cols,
                preferred_element_type=jnp.float32,
            ),
        ],
        axis=1,
    ).astype(jnp.bfloat16)
    input_rows = jnp.concatenate(
        [query_rows_gradient, key_rows_gradient, value_rows_gradient, adapter_grad], axis=1
    )
    grad_normed = scatter_sum(
        columns_product(input_rows, in_parts, part_width), "tensor", minor
    )
    hook = sum_ranks(adapter_grad, "tensor", minor).astype(jnp.bfloat16)
    adapter_term = jnp.stack(
        [
            lax.dot_general(
                pol_normed[c], hook, rows_contraction, preferred_element_type=jnp.float32
            ).astype(jnp.bfloat16)
            for c in range(tensor_size)
        ]
    ).reshape(data_size, full_width // data_size, 2 * rank_size)
    grad_a = scatter_sum(lambda d: take(adapter_term, d), "dp", data_minor)
    narrow = pol_hidden.astype(jnp.float32)
    pre_dot = sum_ranks(jnp.sum(narrow * pre_local * grad_normed, axis=1), "tensor", minor)
    grad_hidden = (
        grad_result
        + pol_scale * pre_local * grad_normed
        - narrow * pol_scale**3 * pre_dot[:, None] / full_width
    )
    return (
        pol_result.astype(jnp.bfloat16),
        ref_result.astype(jnp.bfloat16),
        dpo_loss,
        grad_hidden.astype(jnp.bfloat16),
        grad_a,
        query_factor_gradient,
        value_factor_gradient,
    )


def solution(mesh):
    placed = (
        P("dp", "tensor"),
        P("dp", "tensor"),
        P("dp", "tensor"),
        P("dp"),
        P(),
        P(),
        P(),
        P("dp", "tensor"),
        P("dp", "tensor"),
        P("dp", "tensor"),
        P("dp", "tensor"),
        P("dp", None),
        P("dp", None),
        P(None, "tensor"),
        P(None, "tensor"),
    )
    return jax.shard_map(
        body,
        mesh=mesh,
        in_specs=placed,
        out_specs=(
            P("dp", "tensor"),
            P("dp", "tensor"),
            P(),
            P("dp", "tensor"),
            P("dp", None),
            P(None, "tensor"),
            P(None, "tensor"),
        ),
        check_vma=False,
    )
```
